128 devices in a mesh: sub: 16 (over x, z), fdr: 8 (over y, core).
Axes of the slice: x: 4, y: 4, z: 4, core: 2. Of those that a mesh axis runs over, the one named last changes fastest.
Arguments:
- inverse: bfloat16 [4096, 256, 256], P(('sub', 'fdr')), may hold values from -1 to 1
- cost: float32 [4096, 256, 128], P(('sub', 'fdr')), may hold values from -6 to 6
- lower_limit: float32 [4096, 256], P(('sub', 'fdr')), may hold values from -1.5 to -0.5
- upper_limit: float32 [4096, 256], P(('sub', 'fdr')), may hold values from 0.5 to 1.5
- iface_rows: int32 [4096, 6], P(('sub', 'fdr')), may hold values from 0 to 255, as said below
- substation_of: int32 [4096], P(('sub', 'fdr')), may hold values from 0 to 511, as said below
- live_count: int32 [128], P(('sub', 'fdr')), may hold values from 16 to 32
- reserve_weight: float32 [512], P('sub'), may hold values from 0.5 to 4
- reserve_target: float32 [512, 6, 128], P('sub'), may hold values from -6 to 6
Outputs:
- duals: float32 [4096, 6, 128], P(('sub', 'fdr'))
- consensus: float32 [512, 6, 128], P('sub')
- residual_norms: float32 [5, 2], replicated
- setpoints: float32 [4096, 256, 128], P(('sub', 'fdr'))
The draws below stay inside these ranges and needn't reach their ends.
Inputs may be any that keep to these rules, and one draw needn't show every extreme that they name: `iface_rows`: each feeder's 6 interface rows are distinct. `substation_of`: of one device's 32 slots at most 3 hang from substations of one owner block (substations k * 32 to k * 32 + 31); for each index of fdr some block gets exactly 3 slots from every device with that index. `live_count`: a device's live feeders fill its first slots; the other slots hold unused data.
All inputs are finite; a program needn't handle non-finite values.
Results may differ from the reference program's by a relative error of at most 0.0069.
Values sent between devices are 32-bit elements; how exact they have to be, the bound alone decides.
A program may use at most 128 MiB of HBM per device.

```python
import math
import jax
import jax.numpy as jnp
from jax import lax

KKT = 256
IFC = 6
SC = 128
FDEV = 32
SDEV = 32
ITERS = 5
F = 4096
S = 512
CAP = 3
N_SUB = 16
N_FDR = 8
DEVICES = 128


def draw_inverse(key, part):
    key_a = jax.random.fold_in(key, 11)
    key_b = jax.random.fold_in(key, 12)
    noise_draw = jax.random.normal(key_a, (F, KKT, KKT), jnp.float32)
    symmetric = (noise_draw + jnp.swapaxes(noise_draw, 1, 2)) * (0.25 / KKT ** 0.5)
    diag_vals = jax.random.uniform(key_b, (F, KKT), jnp.float32, 0.3, 0.8)
    identity_matrix = jnp.eye(KKT, dtype=jnp.float32)
    matrix = symmetric + diag_vals[:, :, None] * identity_matrix[None, :, :]
    matrix = jnp.clip(matrix, -1.0, 1.0)
    return matrix.astype(jnp.bfloat16)


def draw_iface_rows(key, part):
    scores = jax.random.randint(jax.random.fold_in(key, 21), (F, KKT), 0, KKT)
    scores = scores * KKT + jnp.arange(KKT, dtype=jnp.int32)[None, :]
    ranking = jnp.argsort(scores, axis=1, stable=True)
    return ranking[:, :IFC].astype(jnp.int32)


def draw_substation_of(key, part):
    slot_total = N_SUB * CAP
    entry = jnp.arange(slot_total, dtype=jnp.int32)
    entry_group = entry // CAP
    column_first = jax.random.randint(jax.random.fold_in(key, 31), (N_FDR,), 0, N_SUB).astype(jnp.int32)
    device_first = jnp.tile(column_first, DEVICES // N_FDR)
    noise_int = jax.random.randint(jax.random.fold_in(key, 32), (DEVICES, slot_total), 0, 65536).astype(jnp.int32)
    priority = entry_group[None, :] == device_first[:, None]
    scores = jnp.where(priority, entry[None, :], (noise_int + 1) * slot_total + entry[None, :])
    ranking = jnp.argsort(scores, axis=1, stable=True)
    chosen = entry_group[ranking[:, :FDEV]]
    shuffle_scores = jax.random.randint(jax.random.fold_in(key, 33), (DEVICES, FDEV), 0, 65536).astype(jnp.int32) * FDEV + jnp.arange(FDEV, dtype=jnp.int32)[None, :]
    shuffle = jnp.argsort(shuffle_scores, axis=1, stable=True)
    groups = jnp.take_along_axis(chosen, shuffle, axis=1)
    within = jax.random.randint(jax.random.fold_in(key, 34), (DEVICES, FDEV), 0, SDEV).astype(jnp.int32)
    return (groups * SDEV + within).reshape(DEVICES * FDEV).astype(jnp.int32)


def set_ends(result, stream_key, low, top_value):
    extent = result.shape
    index_at = [jax.random.randint(jax.random.fold_in(stream_key, axis), (), 0, extent[axis]) for axis in range(len(extent))]
    result = result.at[tuple(index_at)].set(low)
    longest = extent.index(max(extent))
    index_at[longest] = (index_at[longest] + 1) % extent[longest]
    return result.at[tuple(index_at)].set(top_value)


def shard_levels(rng, extent, pieces, least, top_value):
    factor_of, own = 1.0, jax.random.fold_in(rng, 6)
    for position, blocks in pieces:
        draws = jnp.exp(jax.random.uniform(jax.random.fold_in(own, position), (blocks,), jnp.float32, least / len(pieces), top_value / len(pieces)))
        factor_of = factor_of * jnp.repeat(draws, extent[position] // blocks).reshape([-1 if axis == position else 1 for axis in range(len(extent))])
    return factor_of


def normal_values(stream_key, dims, width, limit, cuts=(), held_as=jnp.bfloat16):
    loudness = shard_levels(stream_key, dims, cuts, -0.22, 0.18) if cuts else 1.0
    array = jax.random.normal(stream_key, dims, jnp.float32) * width * loudness
    return jnp.minimum(jnp.maximum(array, -limit), limit).astype(held_as)


def setup_inputs(seed: int = 0) -> dict:
    streams_of = jax.random.split(jax.random.key(seed), 10)
    return {
        "inverse": draw_inverse(jax.random.fold_in(streams_of[9], 71), 0),
        "cost": normal_values(streams_of[1], (F, KKT, SC), 1.0, 6.0, ((0, 128),), jnp.float32),
        "lower_limit": jnp.clip(-1.5 + 1.0 * jax.random.uniform(streams_of[2], (F, KKT), jnp.float32) ** shard_levels(streams_of[2], (F, KKT), ((0, 128),), -0.2, 0.2), -1.5, -0.5),
        "upper_limit": jnp.clip(0.5 + 1.0 * jax.random.uniform(streams_of[3], (F, KKT), jnp.float32) ** shard_levels(streams_of[3], (F, KKT), ((0, 128),), -0.2, 0.2), 0.5, 1.5),
        "iface_rows": draw_iface_rows(jax.random.fold_in(streams_of[9], 71), 0),
        "substation_of": draw_substation_of(jax.random.fold_in(streams_of[9], 71), 0),
        "live_count": set_ends(jax.random.randint(streams_of[6], (DEVICES,), FDEV // 2, FDEV + 1), jax.random.fold_in(streams_of[6], 1), FDEV // 2, FDEV).astype(jnp.int32),
        "reserve_weight": jnp.clip(jnp.exp(math.log(4.0) - 2.0794415 * jax.random.uniform(streams_of[7], (S,), jnp.float32) ** shard_levels(streams_of[7], (S,), ((0, 16),), -0.2, 0.2)), 0.5, 4.0),
        "reserve_target": normal_values(streams_of[8], (S, IFC, SC), 1.0, 6.0, ((0, 16),), jnp.float32),
    }


penalty = 2.0

def solve_block(operands):
    block_inverse, block_rhs = operands
    return jnp.einsum('fkj,fjs->fks', block_inverse.astype(jnp.float32), block_rhs.astype(jnp.float32), precision=lax.Precision.HIGHEST)

def reference(inverse, cost, lower_limit, upper_limit, iface_rows, substation_of, live_count, reserve_weight, reserve_target):
    slot_total = inverse.shape[0]
    slot_number = jnp.arange(slot_total, dtype=jnp.int32) % FDEV
    active = (slot_number < jnp.repeat(live_count, FDEV)).astype(jnp.float32)
    members = jax.ops.segment_sum(active, substation_of, num_segments=S)
    feeder_index = jnp.arange(slot_total, dtype=jnp.int32)[:, None]
    blocks = inverse.reshape(slot_total // FDEV, FDEV, KKT, KKT)
    scaled_dual = jnp.zeros((slot_total, IFC, SC), jnp.float32)
    local_consensus = jnp.zeros((slot_total, IFC, SC), jnp.float32)
    anchor = jnp.zeros((slot_total, KKT, SC), jnp.float32)
    consensus = jnp.zeros((S, IFC, SC), jnp.float32)
    history = []
    for iteration in range(ITERS):
        right_side = (anchor - cost).at[feeder_index, iface_rows].add(penalty * (local_consensus - scaled_dual)).astype(jnp.bfloat16)
        primal = lax.map(solve_block, (blocks, right_side.reshape(slot_total // FDEV, FDEV, KKT, SC))).reshape(slot_total, KKT, SC)
        anchor = jnp.clip(primal, lower_limit[:, :, None], upper_limit[:, :, None])
        boundary = jnp.take_along_axis(primal, iface_rows[:, :, None], axis=1)
        outgoing = (boundary + scaled_dual) * active[:, None, None]
        summed = jax.ops.segment_sum(outgoing, substation_of, num_segments=S)
        new_consensus = (summed + reserve_weight[:, None, None] * reserve_target) / (members + reserve_weight)[:, None, None]
        dual_norm = penalty * jnp.sqrt(jnp.sum(members[:, None, None] * (new_consensus - consensus) ** 2))
        consensus = new_consensus
        local_consensus = consensus[substation_of]
        mismatch = boundary - local_consensus
        scaled_dual = (scaled_dual + mismatch) * active[:, None, None]
        primal_norm = jnp.sqrt(jnp.sum(active[:, None, None] * mismatch ** 2))
        history.append(jnp.stack([primal_norm, dual_norm]))
    return (penalty * scaled_dual, consensus, jnp.stack(history), anchor * active[:, None, None])
```

```python
import functools

import jax
import jax.numpy as jnp
from jax import lax
from jax.experimental import pallas as pl
from jax.experimental.pallas import tpu as pltpu
from jax.sharding import Mesh
from jax.sharding import PartitionSpec as P


ITERS = 5
PENALTY = 2.0
AXES = ("sub_0", "sub_1", "fdr_0", "fdr_1")
SUB = ("sub_0", "sub_1")
F, K, C, Q = 32, 256, 128, 6
OWNERS = 3
CHUNK = 4
MESH = pl.DeviceIdType.MESH
f32, bf16, i32 = jnp.float32, jnp.bfloat16, jnp.int32


def ring(d):
    return min(d, 4 - d)


PLANE = sorted(
    ((dx, dz) for dx in range(4) for dz in range(4)),
    key=lambda t: -(ring(t[0]) + ring(t[1])),
)
ALL = sorted(
    (
        (dx, dz, dy, dc)
        for dx in range(4)
        for dz in range(4)
        for dy in range(4)
        for dc in range(2)
    ),
    key=lambda t: -(ring(t[0]) + ring(t[1]) + ring(t[2])),
)[:-2] + [(0, 0, 0, 1)]


def parts(v):
    hi = v.astype(bf16)
    rest = v - hi.astype(f32)
    mid = rest.astype(bf16)
    low = (rest - mid.astype(f32)).astype(bf16)
    return hi, mid, low


def mm(a, b, dims=(((1,), (0,)), ((), ()))):
    return lax.dot_general(a, b, dims, preferred_element_type=f32)


def kernel(
    inv_hbm, cost_hbm, lo_ref, hi_ref, iface, sub, live_ref, weight, target,
    dual_hbm, cons_hbm, norm_ref, set_hbm,
    mat, cost, lob, hib, part0, cols, coef,
    base0, ai, ci, li, hi_i, lcb, sd, out, ri,
    sbuf, cbuf, rep, rbuf, sdo, idbuf, idin, hot, hot_t,
    rwt, den, memb, rows_new, res, resin, consin, cons, dualb, gv, tab, tabs,
    in_sem, tab_sem, id_s, id_r, c_s, c_r, r_s, r_r, n_s, n_r, k_s, k_r, o_sem,
):
    x, z, y, c = [lax.axis_index(a) for a in AXES]
    me = ((x * 4 + z) * 4 + y) * 2 + c
    k_me = x * 4 + z
    own = (c == 1) & (y < OWNERS)
    part = jnp.where(y < OWNERS, y, 0)
    live = live_ref[0]

    def peer(dx, dz, dy, dc):
        t = (lax.rem(x + dx, 4), lax.rem(z + dz, 4), lax.rem(y + dy, 4), lax.rem(c + dc, 2))
        return t, ((t[0] * 4 + t[1]) * 4 + t[2]) * 2 + t[3]

    def wait(view, sem):
        pltpu.make_async_copy(view, view, sem).wait()

    loads = []
    for j in range(F // CHUNK):
        s = pl.ds(j * CHUNK, CHUNK)
        loads.append(
            (
                pltpu.make_async_copy(inv_hbm.at[s], mat.at[s, pl.ds(0, K), :], in_sem.at[0, j]),
                pltpu.make_async_copy(cost_hbm.at[s], cost.at[s], in_sem.at[1, j]),
            )
        )
    for a, b in loads:
        a.start()
        b.start()
    barrier = pltpu.get_barrier_semaphore()
    for d in ALL:
        pl.semaphore_signal(barrier, inc=1, device_id=peer(*d)[0], device_id_type=MESH)

    gv[...] = lax.broadcasted_iota(i32, (C, C), 0) + 1024
    for f in range(F):
        g = jnp.where(f < live, sub[f] // 32, 64 + f)
        gv[f : f + 1, :] = jnp.full((1, C), g, i32)
    grp = gv[...]
    grp_t = grp.T
    row = lax.broadcasted_iota(i32, (C, C), 0)
    lane = lax.broadcasted_iota(i32, (C, C), 1)
    same = grp == grp_t
    rank = jnp.sum(jnp.where(same & (row < lane), 1, 0), axis=0, keepdims=True)
    pos_row = grp_t[0:1] * 3 + rank
    here = jnp.broadcast_to(pos_row, (C, C)).T == lane
    slot_row = jnp.sum(jnp.where(here, row - F, 0), axis=0, keepdims=True) + F
    pos_row = jnp.minimum(pos_row, 47)
    tab[0:1, :] = slot_row
    tab[1:2, :] = pos_row
    to_smem = pltpu.make_async_copy(tab, tabs, tab_sem)
    to_smem.start()

    zero8 = jnp.zeros((F, 8, C), f32)
    for ref in (ci, li, hi_i, lcb, sd):
        ref[...] = zero8
    out[F] = jnp.zeros((8, C), f32)
    to_smem.wait()

    def slot_at(n):
        return jnp.clip(tabs[0, n], 0, F)

    for n in range(48):
        s = slot_at(n)
        number = jnp.where(s < F, (sub[jnp.minimum(s, F - 1)] % 32).astype(f32), -1000.0)
        idbuf[2 * n : 2 * n + 1, :] = jnp.full((1, C), number, f32)
        idbuf[2 * n + 1 : 2 * n + 2, :] = jnp.full((1, C), number + 32.0, f32)

    pl.semaphore_wait(barrier, 127)

    def to_owners(source, dest, first, s_sem, r_sem, self_copy):
        for dx, dz in PLANE:
            tx, tz = lax.rem(x + dx, 4), lax.rem(z + dz, 4)
            k = tx * 4 + tz
            for o in (2, 1, 0):
                copy = pltpu.make_async_remote_copy(
                    source(o, k),
                    dest.at[pl.ds(first + me * 6, 6), :],
                    s_sem,
                    r_sem,
                    device_id=(tx, tz, o, 1),
                    device_id_type=MESH,
                )
                if (dx, dz) == (0, 0):
                    pl.when(jnp.logical_not((y == o) & (c == 1)))(copy.start)
                else:
                    copy.start()

        @pl.when(own)
        def _():
            self_copy()

    def id_self():
        for i in range(6):
            idin[pl.ds(me * 6 + i, 1), :] = idbuf[pl.ds(k_me * 6 + i, 1), :]

    to_owners(lambda o, k: idbuf.at[pl.ds(k * 6, 6), :], idin, 0, id_s, id_r, id_self)

    def wait_48(view, sem):
        @pl.when(own)
        def _():
            wait(view.at[pl.ds(0, 47 * 6), :], sem)

        @pl.when(jnp.logical_not(own))
        def _():
            wait(view.at[pl.ds(0, 48 * 6), :], sem)

    lane16 = lax.broadcasted_iota(i32, (16, K), 1)
    row16 = lax.broadcasted_iota(i32, (16, K), 0)

    def prepare(f):
        at = jnp.full((16, K), -1, i32)
        for q in range(Q):
            at = jnp.where(row16 == q, iface[f, q], at)
        pick32 = jnp.where(lane16 == at, 1.0, 0.0)
        pick = pick32.astype(bf16)
        keep = (1.0 - jnp.sum(pick32, axis=0, keepdims=True)).astype(bf16)
        inverse = mat[f, 0:K, :]
        col = mm(inverse, pick, (((1,), (1,)), ((), ()))).astype(bf16)
        cols[f] = col
        masked = inverse * keep
        mat[f, 0:K, :] = masked
        mat[f, K : K + 16, :] = mm(pick, masked).astype(bf16)
        cross = mm(pick, col)
        for q in range(Q):
            coef[f, q] = jnp.broadcast_to(cross[0:8, q : q + 1], (8, C))
        lob[f] = jnp.broadcast_to(lo_ref[pl.ds(f, 1), :], (C, K)).T
        hib[f] = jnp.broadcast_to(hi_ref[pl.ds(f, 1), :], (C, K)).T
        for q in range(Q):
            r = iface[f, q]
            ci[f, q : q + 1, :] = cost[f, pl.ds(r, 1), :]
            li[f, q : q + 1, :] = lob[f, pl.ds(r, 1), :]
            hi_i[f, q : q + 1, :] = hib[f, pl.ds(r, 1), :]
        ai[f] = -ci[f]
        solve(f, (-cost[f]).astype(bf16))

    def solve(f, base):
        both = mm(mat[f], base)
        part0[f] = both[0:K]
        base0[f] = both[K : K + 8]

    def chunk_loop(body):
        def step(j, carry):
            for i in range(CHUNK):
                body(j * CHUNK + i)
            return carry

        lax.fori_loop(0, F // CHUNK, step, 0)

    for a, b in loads:
        a.wait()
        b.wait()
    chunk_loop(prepare)

    def exchange(t):
        half_at = pl.multiple_of(lax.rem(t, 2) * 768, 768)
        for f in range(F):
            act = jnp.where(f < live, 1.0, 0.0)
            rhs = (ai[f] + PENALTY * (lcb[f] - sd[f])).astype(bf16).astype(f32)
            ri[f] = rhs
            boundary = base0[f]
            for q in range(Q):
                boundary = boundary + coef[f, q] * jnp.broadcast_to(rhs[q : q + 1, :], (8, C))
            out[f] = (boundary + sd[f]) * act
            anchor = jnp.minimum(jnp.maximum(boundary, li[f]), hi_i[f])
            ai[f] = anchor - ci[f]
        for n in range(48):
            v = out[slot_at(n)]
            for o in range(OWNERS):
                sbuf[96 * o + 2 * n : 96 * o + 2 * n + 2, :] = v[2 * o : 2 * o + 2, :]

        def self_copy():
            for i in range(6):
                cbuf[pl.ds(half_at + me * 6 + i, 1), :] = sbuf[pl.ds(part * 96 + k_me * 6 + i, 1), :]

        to_owners(
            lambda o, k: sbuf.at[pl.ds(o * 96 + k * 6, 6), :], cbuf, half_at, c_s, c_r, self_copy
        )

        def primal_of(f):
            primal = part0[f] + mm(cols[f, :, 0:8], ri[f].astype(bf16))
            return jnp.minimum(jnp.maximum(primal, lob[f]), hib[f])

        @pl.when(t < ITERS - 1)
        def _():
            def advance(f):
                solve(f, (primal_of(f) - cost[f]).astype(bf16))

            chunk_loop(advance)

        @pl.when(t == ITERS - 1)
        def _():
            def last(f):
                part0[f] = primal_of(f) * jnp.where(f < live, 1.0, 0.0)

            chunk_loop(last)
            pltpu.make_async_copy(part0, set_hbm, o_sem.at[0]).start()

        @pl.when(own & (t == 0))
        def _():
            wait(idin.at[pl.ds(0, 127 * 6), :], id_r)
            lanes = lax.broadcasted_iota(i32, (768, 256), 1)
            want = jnp.where(lanes < 192, lax.rem(lanes, 64), -1).astype(f32)
            ids = idin[...]
            h = jnp.where(jnp.concatenate([ids, ids], axis=1) == want, 1.0, 0.0)
            hot[...] = h.astype(bf16)
            ht = h[:, 0:C].T[0:64, :]
            hot_t[...] = ht.astype(bf16)
            count = mm(ht.astype(bf16), jnp.ones((768, C), bf16))
            memb[...] = count
            for s in range(32):
                w = weight[s]
                for q in range(2):
                    r = s + 32 * q
                    rwt[r : r + 1, :] = w * target[s, pl.ds(2 * part + q, 1), :]
                    den[r : r + 1, :] = memb[r : r + 1, :] + w
            sdo[...] = jnp.zeros((768, C), f32)
            rows_new[...] = jnp.zeros((64, C), f32)
            res[...] = jnp.zeros((8, C), f32)

        @pl.when(own)
        def _():
            wait(cbuf.at[pl.ds(half_at, 127 * 6), :], c_r)
            arrived = cbuf.at[pl.ds(half_at, 768), :]
            sums = None
            for a in parts(arrived[...]):
                term = mm(hot_t[...], a)
                sums = term if sums is None else sums + term
            new = (sums + rwt[...]) / den[...]
            diff = new - rows_new[...]
            rows_new[...] = new
            triple = jnp.concatenate([*parts(new), jnp.zeros((64, C), bf16)], axis=0)
            back = mm(hot[...], triple)
            rep[...] = back
            for d in ALL:
                to, number = peer(*d)
                pltpu.make_async_remote_copy(
                    rep.at[pl.ds(number * 6, 6), :],
                    rbuf.at[pl.ds(part * 96 + k_me * 6, 6), :],
                    r_s,
                    r_r,
                    device_id=to,
                    device_id_type=MESH,
                ).start()
            for i in range(6):
                rbuf[pl.ds(part * 96 + k_me * 6 + i, 1), :] = rep[pl.ds(me * 6 + i, 1), :]
            next_sd = arrived[...] - rep[...]
            miss = next_sd - sdo[...]
            sdo[...] = next_sd
            primal_sum = jnp.sum(miss * miss, axis=0, keepdims=True)
            dual_sum = jnp.sum(memb[...] * (diff * diff), axis=0, keepdims=True)
            half = lax.broadcasted_iota(i32, (1, C), 1) < 64
            folded = jnp.where(
                half,
                primal_sum + pltpu.roll(primal_sum, 64, 1),
                dual_sum + pltpu.roll(dual_sum, 64, 1),
            )
            res[...] = jnp.where(lax.broadcasted_iota(i32, (8, C), 0) == t, folded, res[...])

            @pl.when(t == ITERS - 1)
            def _():
                for dx, dz, dy, dc in ALL:
                    to, number = peer(dx, dz, dy, dc)
                    if (dx, dz) == (0, 0):
                        pltpu.make_async_remote_copy(
                            rows_new, consin.at[part], k_s, k_r, device_id=to, device_id_type=MESH
                        ).start()
                    pltpu.make_async_remote_copy(
                        res, resin.at[part * 16 + k_me], n_s, n_r, device_id=to, device_id_type=MESH
                    ).start()
                resin[part * 16 + k_me] = res[...]
                consin[part] = rows_new[...]

            wait(rep.at[pl.ds(0, 127 * 6), :], r_s)

        wait_48(rbuf, r_r)

        for f in range(F):
            at = 2 * jnp.clip(tabs[1, f], 0, 47)
            for o in range(OWNERS):
                for q in range(2):
                    r = 2 * o + q
                    lcb[f, r : r + 1, :] = rbuf[pl.ds(96 * o + at + q, 1), :]
        for f in range(F):
            act = jnp.where(f < live, 1.0, 0.0)
            sd[f] = out[f] - lcb[f] * act

        wait_48(sbuf, c_s)
        return 0

    lax.fori_loop(0, ITERS, lambda t, carry: exchange(t), 0)

    dualb[...] = PENALTY * sd[:, 0:Q, :]
    dual_out = pltpu.make_async_copy(dualb, dual_hbm, o_sem.at[1])
    dual_out.start()

    @pl.when(own)
    def _():
        wait(consin.at[pl.ds(0, 2)], k_r)
        wait(resin.at[pl.ds(0, 47)], n_r)

    @pl.when(jnp.logical_not(own))
    def _():
        wait(consin, k_r)
        wait(resin, n_r)

    for o in range(OWNERS):
        for q in range(2):
            cons[:, 2 * o + q, :] = consin[o, 32 * q : 32 * q + 32, :]
    cons_out = pltpu.make_async_copy(cons, cons_hbm, o_sem.at[2])
    cons_out.start()
    total = jnp.sum(resin[...], axis=0)
    lane8 = lax.broadcasted_iota(i32, (8, C), 1)
    primal = jnp.sum(jnp.where(lane8 < 64, total, 0.0), axis=1, keepdims=True)
    dual = jnp.sum(jnp.where(lane8 < 64, 0.0, total), axis=1, keepdims=True)
    norms = jnp.where(lane8 == 0, jnp.sqrt(primal), PENALTY * jnp.sqrt(dual))
    norm_ref[...] = norms[0:ITERS, 0:2]

    @pl.when(own)
    def _():
        wait(cbuf.at[pl.ds(0, 7 * 64), :], k_s)
        wait(cbuf.at[pl.ds(0, 127 * 8), :], n_s)

    wait_48(idin, id_s)
    pltpu.make_async_copy(part0, set_hbm, o_sem.at[0]).wait()
    dual_out.wait()
    cons_out.wait()


def shards(*operands):
    vmem = functools.partial(pltpu.VMEM, dtype=f32)
    anyspace = pl.BlockSpec(memory_space=pl.ANY)
    on_vmem = pl.BlockSpec(memory_space=pltpu.VMEM)
    on_smem = pl.BlockSpec(memory_space=pltpu.SMEM)
    dma = pltpu.SemaphoreType.DMA
    return pl.pallas_call(
        kernel,
        out_shape=(
            jax.ShapeDtypeStruct((F, Q, C), f32),
            jax.ShapeDtypeStruct((32, Q, C), f32),
            jax.ShapeDtypeStruct((ITERS, 2), f32),
            jax.ShapeDtypeStruct((F, K, C), f32),
        ),
        in_specs=[anyspace, anyspace, on_vmem, on_vmem, on_smem, on_smem, on_smem, on_smem, on_vmem],
        out_specs=(anyspace, anyspace, on_vmem, anyspace),
        scratch_shapes=[
            pltpu.VMEM((F, K + 16, K), bf16),
            vmem((F, K, C)),
            vmem((F, K, C)),
            vmem((F, K, C)),
            vmem((F, K, C)),
            pltpu.VMEM((F, K, 16), bf16),
            vmem((F, Q, 8, C)),
            vmem((F, 8, C)),
            vmem((F, 8, C)),
            vmem((F, 8, C)),
            vmem((F, 8, C)),
            vmem((F, 8, C)),
            vmem((F, 8, C)),
            vmem((F, 8, C)),
            vmem((F + 1, 8, C)),
            vmem((F, 8, C)),
            vmem((OWNERS * 96, C)),
            vmem((2 * 768, C)),
            vmem((768, C)),
            vmem((OWNERS * 96, C)),
            vmem((768, C)),
            vmem((96, C)),
            vmem((768, C)),
            pltpu.VMEM((768, 256), bf16),
            pltpu.VMEM((64, 768), bf16),
            vmem((64, C)),
            vmem((64, C)),
            vmem((64, C)),
            vmem((64, C)),
            vmem((8, C)),
            vmem((48, 8, C)),
            vmem((OWNERS, 64, C)),
            vmem((32, Q, C)),
            vmem((F, Q, C)),
            pltpu.VMEM((C, C), i32),
            pltpu.VMEM((2, C), i32),
            pltpu.SMEM((2, C), i32),
            dma((2, F // CHUNK)),
            dma,
            dma,
            dma,
            dma,
            dma,
            dma,
            dma,
            dma,
            dma,
            dma,
            dma,
            dma((3,)),
        ],
        compiler_params=pltpu.CompilerParams(
            collective_id=0, has_side_effects=True, vmem_limit_bytes=58 * 2**20
        ),
    )(*operands)


def solution(mesh):
    torus = Mesh(mesh.devices.reshape(4, 4, 4, 2), AXES)
    placed = (
        P(AXES, None, None),
        P(AXES, None, None),
        P(AXES, None),
        P(AXES, None),
        P(AXES, None),
        P(AXES),
        P(AXES),
        P(SUB),
        P(SUB, None, None),
    )
    return jax.shard_map(
        shards,
        mesh=torus,
        in_specs=placed,
        out_specs=(P(AXES, None, None), P(SUB, None, None), P(), P(AXES, None, None)),
        check_vma=False,
    )
```

```python
import functools

import jax
import jax.numpy as jnp
from jax import lax
from jax.experimental import pallas as pl
from jax.experimental.pallas import tpu as pltpu
from jax.sharding import Mesh
from jax.sharding import PartitionSpec as P


ITERS = 5
PENALTY = 2.0
AXES = ("sub_0", "sub_1", "fdr_0", "fdr_1")
SUB = ("sub_0", "sub_1")
F, K, C, Q = 32, 256, 128, 6
OWNERS = 3
CHUNK = 8
MESH = pl.DeviceIdType.MESH
NT = (((1,), (1,)), ((), ()))
f32, bf16, i32 = jnp.float32, jnp.bfloat16, jnp.int32


def ring(d):
    return min(d, 4 - d)


PLANE = sorted(
    ((dx, dz) for dx in range(4) for dz in range(4)),
    key=lambda t: -(ring(t[0]) + ring(t[1])),
)
ALL = sorted(
    (
        (dx, dz, dy, dc)
        for dx in range(4)
        for dz in range(4)
        for dy in range(4)
        for dc in range(2)
    ),
    key=lambda t: -(ring(t[0]) + ring(t[1]) + ring(t[2])),
)[:-2] + [(0, 0, 0, 1)]


def parts(v):
    hi = v.astype(bf16)
    rest = v - hi.astype(f32)
    mid = rest.astype(bf16)
    low = (rest - mid.astype(f32)).astype(bf16)
    return hi, mid, low


def mm(a, b, dims=(((1,), (0,)), ((), ()))):
    return lax.dot_general(a, b, dims, preferred_element_type=f32)


def kernel(
    inv_hbm, cost_hbm, lo_hbm, hi_hbm, iface_hbm, sub_hbm, live_hbm, weight_hbm, target_hbm,
    dual_ref, cons_ref, norm_ref, part0,
    mat, cost, lob, hib, cols, coef,
    base0, ai, ci, li, hi_i, lcb, sd, out, ri,
    sbuf, cbuf, rep, rbuf, sdo, idbuf, idin, hot, hot_t,
    rwt, den, memb, rows_new, res, resin, consin, gv, tab, tabs,
    lo_ref, hi_ref, iface, sub, live_ref, weight, target, bnd,
    in_sem, arg_sem, tab_sem, id_s, id_r, c_s, c_r, r_s, r_r, n_s, n_r, k_s, k_r,
):
    x, z, y, c = [lax.axis_index(a) for a in AXES]
    me = ((x * 4 + z) * 4 + y) * 2 + c
    k_me = x * 4 + z
    own = (c == 1) & (y < OWNERS)
    part = jnp.where(y < OWNERS, y, 0)

    def peer(dx, dz, dy, dc):
        t = (lax.rem(x + dx, 4), lax.rem(z + dz, 4), lax.rem(y + dy, 4), lax.rem(c + dc, 2))
        return t, ((t[0] * 4 + t[1]) * 4 + t[2]) * 2 + t[3]

    def wait(view, sem):
        pltpu.make_async_copy(view, view, sem).wait()

    small = [
        pltpu.make_async_copy(a, b, arg_sem.at[i])
        for i, (a, b) in enumerate(
            (
                (sub_hbm, sub),
                (live_hbm, live_ref),
                (iface_hbm, iface),
                (weight_hbm, weight),
                (lo_hbm, lo_ref),
                (hi_hbm, hi_ref),
                (target_hbm, target),
            )
        )
    ]

    def loads(j):
        s = pl.ds(j * CHUNK, CHUNK)
        return (
            pltpu.make_async_copy(inv_hbm.at[s], mat.at[s, pl.ds(0, K), :], in_sem.at[0, j]),
            pltpu.make_async_copy(cost_hbm.at[s], cost.at[s], in_sem.at[1, j]),
        )

    for copy in small[:3]:
        copy.start()
    for j in range(F // CHUNK):
        for copy in loads(j):
            copy.start()
    for copy in small[3:]:
        copy.start()
    barrier = pltpu.get_barrier_semaphore()
    for d in ALL:
        pl.semaphore_signal(barrier, inc=1, device_id=peer(*d)[0], device_id_type=MESH)

    for copy in small[:3]:
        copy.wait()
    live = live_ref[0]

    gv[...] = lax.broadcasted_iota(i32, (C, C), 0) + 1024
    for f in range(F):
        g = jnp.where(f < live, sub[f] // 32, 64 + f)
        gv[f : f + 1, :] = jnp.full((1, C), g, i32)
    grp = gv[...]
    grp_t = grp.T
    row = lax.broadcasted_iota(i32, (C, C), 0)
    lane = lax.broadcasted_iota(i32, (C, C), 1)
    same = grp == grp_t
    rank = jnp.sum(jnp.where(same & (row < lane), 1, 0), axis=0, keepdims=True)
    pos_row = grp_t[0:1] * 3 + rank
    here = jnp.broadcast_to(pos_row, (C, C)).T == lane
    slot_row = jnp.sum(jnp.where(here, row - F, 0), axis=0, keepdims=True) + F
    pos_row = jnp.minimum(pos_row, 47)
    tab[0:1, :] = slot_row
    tab[1:2, :] = pos_row
    to_smem = pltpu.make_async_copy(tab, tabs, tab_sem)
    to_smem.start()

    zero8 = jnp.zeros((F, 8, C), f32)
    for ref in (ai, ci, li, hi_i, lcb, sd):
        ref[...] = zero8
    coef[...] = jnp.zeros((F, Q, 8, C), f32)
    out[F] = jnp.zeros((8, C), f32)
    def slot_at(n):
        return jnp.clip(tabs[0, n], 0, F)

    def to_owners(source, dest, first, s_sem, r_sem, self_copy):
        for dx, dz in PLANE:
            tx, tz = lax.rem(x + dx, 4), lax.rem(z + dz, 4)
            k = tx * 4 + tz
            for o in (2, 1, 0):
                copy = pltpu.make_async_remote_copy(
                    source(o, k),
                    dest.at[pl.ds(first + me * 6, 6), :],
                    s_sem,
                    r_sem,
                    device_id=(tx, tz, o, 1),
                    device_id_type=MESH,
                )
                if (dx, dz) == (0, 0):
                    pl.when(jnp.logical_not((y == o) & (c == 1)))(copy.start)
                else:
                    copy.start()

        @pl.when(own)
        def _():
            self_copy()

    def wait_48(view, sem):
        @pl.when(own)
        def _():
            wait(view.at[pl.ds(0, 47 * 6), :], sem)

        @pl.when(jnp.logical_not(own))
        def _():
            wait(view.at[pl.ds(0, 48 * 6), :], sem)

    lane16 = lax.broadcasted_iota(i32, (16, K), 1)
    row16 = lax.broadcasted_iota(i32, (16, K), 0)

    def picks(f):
        at = jnp.full((16, K), -1, i32)
        for q in range(Q):
            at = jnp.where(row16 == q, iface[q, f], at)
        pick = jnp.where(lane16 == at, 1.0, 0.0)
        return pick.astype(bf16), 1.0 - jnp.sum(pick, axis=0, keepdims=True)

    def prepare(f):
        pick, _ = picks(f)
        rows = mm(pick, mat[f, 0:K, :]).astype(bf16)
        mat[f, K : K + 16, :] = rows
        base0[f] = mm(rows, (-cost[f]).astype(bf16))[0:8]

    def complete(f):
        pick, keep = picks(f)
        cols[f] = mm(mat[f, 0:K, :], pick, NT).astype(bf16)
        rows = mat[f, K : K + 16, :]
        cross = mm(rows, pick, NT)
        mat[f, K : K + 16, :] = rows * keep.astype(bf16)
        for q in range(Q):
            coef[f, q] = jnp.broadcast_to(cross[0:8, q : q + 1], (8, C))
        lob[f] = jnp.broadcast_to(lo_ref[pl.ds(f, 1), :], (C, K)).T
        hib[f] = jnp.broadcast_to(hi_ref[pl.ds(f, 1), :], (C, K)).T
        for q in range(Q):
            r = iface[q, f]
            ci[f, q : q + 1, :] = cost[f, pl.ds(r, 1), :]
            li[f, q : q + 1, :] = lob[f, pl.ds(r, 1), :]
            hi_i[f, q : q + 1, :] = hib[f, pl.ds(r, 1), :]

    def first(f):
        _, keep = picks(f)
        inverse = mat[f, 0:K, :]
        primal = mm(inverse, (-cost[f]).astype(bf16))
        mat[f, 0:K, :] = inverse * keep.astype(bf16)
        anchor = jnp.minimum(jnp.maximum(primal, lob[f]), hib[f])
        solve(f, (anchor - cost[f]).astype(bf16))

    def solve(f, base):
        both = mm(mat[f], base)
        part0[f] = both[0:K]
        base0[f] = both[K : K + 8]

    def chunk_loop(body, arrive=False):
        def step(j, carry):
            if arrive:
                for copy in loads(j):
                    copy.wait()
            for i in range(CHUNK):
                body(j * CHUNK + i)
            return carry

        lax.fori_loop(0, F // CHUNK, step, 0)

    chunk_loop(prepare, arrive=True)

    to_smem.wait()
    for n in range(48):
        s = slot_at(n)
        number = jnp.where(s < F, (sub[jnp.minimum(s, F - 1)] % 32).astype(f32), -1000.0)
        idbuf[2 * n : 2 * n + 1, :] = jnp.full((1, C), number, f32)
        idbuf[2 * n + 1 : 2 * n + 2, :] = jnp.full((1, C), number + 32.0, f32)
    pl.semaphore_wait(barrier, 127)

    def id_self():
        for i in range(6):
            idin[pl.ds(me * 6 + i, 1), :] = idbuf[pl.ds(k_me * 6 + i, 1), :]

    to_owners(lambda o, k: idbuf.at[pl.ds(k * 6, 6), :], idin, 0, id_s, id_r, id_self)
    for copy in small[3:]:
        copy.wait()

    def exchange(t):
        half_at = pl.multiple_of(lax.rem(t, 2) * 768, 768)
        for f in range(F):
            act = jnp.where(f < live, 1.0, 0.0)
            rhs = (ai[f] + PENALTY * (lcb[f] - sd[f])).astype(bf16).astype(f32)
            ri[f] = rhs
            boundary = base0[f]
            for q in range(Q):
                boundary = boundary + coef[f, q] * jnp.broadcast_to(rhs[q : q + 1, :], (8, C))
            out[f] = (boundary + sd[f]) * act
            bnd[f] = boundary
        for n in range(48):
            v = out[slot_at(n)]
            for o in range(OWNERS):
                sbuf[96 * o + 2 * n : 96 * o + 2 * n + 2, :] = v[2 * o : 2 * o + 2, :]

        def self_copy():
            for i in range(6):
                cbuf[pl.ds(half_at + me * 6 + i, 1), :] = sbuf[pl.ds(part * 96 + k_me * 6 + i, 1), :]

        to_owners(
            lambda o, k: sbuf.at[pl.ds(o * 96 + k * 6, 6), :], cbuf, half_at, c_s, c_r, self_copy
        )

        def primal_of(f):
            primal = part0[f] + mm(cols[f, :, 0:8], ri[f].astype(bf16))
            return jnp.minimum(jnp.maximum(primal, lob[f]), hib[f])

        @pl.when(t == 0)
        def _():
            chunk_loop(complete)

        @pl.when((t > 0) & (t < ITERS - 1))
        def _():
            def advance(f):
                solve(f, (primal_of(f) - cost[f]).astype(bf16))

            chunk_loop(advance)

        @pl.when(t == ITERS - 1)
        def _():
            def last(f):
                part0[f] = primal_of(f) * jnp.where(f < live, 1.0, 0.0)

            chunk_loop(last)

        @pl.when(own & (t == 0))
        def _():
            wait(idin.at[pl.ds(0, 127 * 6), :], id_r)
            lanes = lax.broadcasted_iota(i32, (768, 256), 1)
            want = jnp.where(lanes < 192, lax.rem(lanes, 64), -1).astype(f32)
            ids = idin[...]
            h = jnp.where(jnp.concatenate([ids, ids], axis=1) == want, 1.0, 0.0)
            hot[...] = h.astype(bf16)
            ht = h[:, 0:C].T[0:64, :]
            hot_t[...] = ht.astype(bf16)
            count = mm(ht.astype(bf16), jnp.ones((768, C), bf16))
            memb[...] = count
            for s in range(32):
                w = weight[s]
                for q in range(2):
                    r = s + 32 * q
                    rwt[r : r + 1, :] = w * target[2 * part + q, s : s + 1, :]
                    den[r : r + 1, :] = memb[r : r + 1, :] + w
            sdo[...] = jnp.zeros((768, C), f32)
            rows_new[...] = jnp.zeros((64, C), f32)
            res[...] = jnp.zeros((1, C), f32)

        for f in range(F):
            ai[f] = jnp.minimum(jnp.maximum(bnd[f], li[f]), hi_i[f]) - ci[f]

        @pl.when(own)
        def _():
            wait(cbuf.at[pl.ds(half_at, 127 * 6), :], c_r)
            arrived = cbuf.at[pl.ds(half_at, 768), :]
            sums = None
            for a in parts(arrived[...]):
                term = mm(hot_t[...], a)
                sums = term if sums is None else sums + term
            new = (sums + rwt[...]) / den[...]
            diff = new - rows_new[...]
            rows_new[...] = new
            triple = jnp.concatenate([*parts(new), jnp.zeros((64, C), bf16)], axis=0)
            back = mm(hot[...], triple)
            rep[...] = back
            for d in ALL:
                to, number = peer(*d)
                pltpu.make_async_remote_copy(
                    rep.at[pl.ds(number * 6, 6), :],
                    rbuf.at[pl.ds(part * 96 + k_me * 6, 6), :],
                    r_s,
                    r_r,
                    device_id=to,
                    device_id_type=MESH,
                ).start()
            for i in range(6):
                rbuf[pl.ds(part * 96 + k_me * 6 + i, 1), :] = rep[pl.ds(me * 6 + i, 1), :]
            next_sd = arrived[...] - rep[...]
            miss = next_sd - sdo[...]
            sdo[...] = next_sd
            primal_sum = jnp.sum(miss * miss, axis=0, keepdims=True)
            dual_sum = jnp.sum(memb[...] * (diff * diff), axis=0, keepdims=True)
            lane1 = lax.broadcasted_iota(i32, (1, C), 1)
            for at, value in ((t, primal_sum), (t + 64, dual_sum)):
                value = jnp.broadcast_to(jnp.sum(value, axis=1, keepdims=True), (1, C))
                res[...] = jnp.where(lane1 == at, value, res[...])

            @pl.when(t == ITERS - 1)
            def _():
                for dx, dz, dy, dc in ALL:
                    to, number = peer(dx, dz, dy, dc)
                    if (dx, dz) == (0, 0):
                        pltpu.make_async_remote_copy(
                            rows_new, consin.at[part], k_s, k_r, device_id=to, device_id_type=MESH
                        ).start()
                    pltpu.make_async_remote_copy(
                        res, resin.at[pl.ds(part * 16 + k_me, 1), :], n_s, n_r, device_id=to, device_id_type=MESH
                    ).start()
                resin[pl.ds(part * 16 + k_me, 1), :] = res[...]
                consin[part] = rows_new[...]

            wait(rep.at[pl.ds(0, 127 * 6), :], r_s)

        @pl.when(t == 0)
        def _():
            chunk_loop(first)

        wait_48(rbuf, r_r)

        for f in range(F):
            at = 2 * jnp.clip(tabs[1, f], 0, 47)
            for o in range(OWNERS):
                for q in range(2):
                    r = 2 * o + q
                    lcb[f, r : r + 1, :] = rbuf[pl.ds(96 * o + at + q, 1), :]
        for f in range(F):
            act = jnp.where(f < live, 1.0, 0.0)
            sd[f] = out[f] - lcb[f] * act

        wait_48(sbuf, c_s)
        return 0

    lax.fori_loop(0, ITERS, lambda t, carry: exchange(t), 0)

    for q in range(Q):
        dual_ref[q] = PENALTY * sd[:, q, :]

    @pl.when(own)
    def _():
        wait(consin.at[pl.ds(0, 2)], k_r)
        wait(resin.at[pl.ds(0, 47), :], n_r)

    @pl.when(jnp.logical_not(own))
    def _():
        wait(consin, k_r)
        wait(resin, n_r)

    for o in range(OWNERS):
        for q in range(2):
            cons_ref[2 * o + q] = consin[o, 32 * q : 32 * q + 32, :]
    root = jnp.sqrt(jnp.sum(resin[...], axis=0, keepdims=True))
    norm_ref[0:1, :] = root[:, 0:ITERS]
    norm_ref[1:2, :] = PENALTY * root[:, 64 : 64 + ITERS]

    @pl.when(own)
    def _():
        wait(cbuf.at[pl.ds(0, 7 * 64), :], k_s)
        wait(cbuf.at[pl.ds(0, 127), :], n_s)

    wait_48(idin, id_s)


def shards(inverse, cost, lower, upper, iface, sub, live, weight, target):
    operands = (inverse, cost, lower, upper, iface.T, sub, live, weight, target.transpose(1, 0, 2))
    vmem = functools.partial(pltpu.VMEM, dtype=f32)
    anyspace = pl.BlockSpec(memory_space=pl.ANY)
    on_vmem = pl.BlockSpec(memory_space=pltpu.VMEM)
    dma = pltpu.SemaphoreType.DMA
    shapes = ((Q, F, C), (Q, 32, C), (2, ITERS), (F, K, C))
    duals, consensus, norms, setpoints = pl.pallas_call(
        kernel,
        out_shape=tuple(vmem(shape) for shape in shapes),
        in_specs=[anyspace] * 9,
        out_specs=(on_vmem,) * 4,
        scratch_shapes=[
            pltpu.VMEM((F, K + 16, K), bf16),
            vmem((F, K, C)),
            vmem((F, K, C)),
            vmem((F, K, C)),
            pltpu.VMEM((F, K, 16), bf16),
            vmem((F, Q, 8, C)),
            vmem((F, 8, C)),
            vmem((F, 8, C)),
            vmem((F, 8, C)),
            vmem((F, 8, C)),
            vmem((F, 8, C)),
            vmem((F, 8, C)),
            vmem((F, 8, C)),
            vmem((F + 1, 8, C)),
            vmem((F, 8, C)),
            vmem((OWNERS * 96, C)),
            vmem((2 * 768, C)),
            vmem((768, C)),
            vmem((OWNERS * 96, C)),
            vmem((768, C)),
            vmem((96, C)),
            vmem((768, C)),
            pltpu.VMEM((768, 256), bf16),
            pltpu.VMEM((64, 768), bf16),
            vmem((64, C)),
            vmem((64, C)),
            vmem((64, C)),
            vmem((64, C)),
            vmem((1, C)),
            vmem((48, C)),
            vmem((OWNERS, 64, C)),
            pltpu.VMEM((C, C), i32),
            pltpu.VMEM((2, C), i32),
            pltpu.SMEM((2, C), i32),
            vmem((F, K)),
            vmem((F, K)),
            pltpu.SMEM((Q, F), i32),
            pltpu.SMEM((F,), i32),
            pltpu.SMEM((1,), i32),
            pltpu.SMEM((32,), f32),
            vmem((Q, 32, C)),
            vmem((F, 8, C)),
            dma((2, F // CHUNK)),
            dma((7,)),
            dma,
            dma,
            dma,
            dma,
            dma,
            dma,
            dma,
            dma,
            dma,
            dma,
            dma,
        ],
        compiler_params=pltpu.CompilerParams(
            collective_id=0, has_side_effects=True, vmem_limit_bytes=58 * 2**20
        ),
    )(*operands)
    return duals.transpose(1, 0, 2), consensus.transpose(1, 0, 2), norms.T, setpoints


def solution(mesh):
    torus = Mesh(mesh.devices.reshape(4, 4, 4, 2), AXES)
    placed = (
        P(AXES, None, None),
        P(AXES, None, None),
        P(AXES, None),
        P(AXES, None),
        P(AXES, None),
        P(AXES),
        P(AXES),
        P(SUB),
        P(SUB, None, None),
    )
    return jax.shard_map(
        shards,
        mesh=torus,
        in_specs=placed,
        out_specs=(P(AXES, None, None), P(SUB, None, None), P(), P(AXES, None, None)),
        check_vma=False,
    )
```

```python
import functools

import jax
import jax.numpy as jnp
from jax import lax
from jax.experimental import pallas as pl
from jax.experimental.pallas import tpu as pltpu
from jax.sharding import Mesh
from jax.sharding import PartitionSpec as P


ITERS = 5
PENALTY = 2.0
AXES = ("sub_0", "sub_1", "fdr_0", "fdr_1")
SUB = ("sub_0", "sub_1")
F, K, C, Q = 32, 256, 128, 6
OWNERS = 3
CHUNK = 8
MESH = pl.DeviceIdType.MESH
NT = (((1,), (1,)), ((), ()))
f32, bf16, i32 = jnp.float32, jnp.bfloat16, jnp.int32


def ring(d):
    return min(d, 4 - d)


PLANE = sorted(
    ((dx, dz) for dx in range(4) for dz in range(4)),
    key=lambda t: -(ring(t[0]) + ring(t[1])),
)
ALL = sorted(
    (
        (dx, dz, dy, dc)
        for dx in range(4)
        for dz in range(4)
        for dy in range(4)
        for dc in range(2)
    ),
    key=lambda t: -(ring(t[0]) + ring(t[1]) + ring(t[2])),
)[:-2] + [(0, 0, 0, 1)]


def parts(v):
    hi = v.astype(bf16)
    rest = v - hi.astype(f32)
    mid = rest.astype(bf16)
    low = (rest - mid.astype(f32)).astype(bf16)
    return hi, mid, low


def mm(a, b, dims=(((1,), (0,)), ((), ()))):
    return lax.dot_general(a, b, dims, preferred_element_type=f32)


def kernel(
    inv_hbm, cost_hbm, lo_hbm, hi_hbm, iface_hbm, sub_hbm, live_hbm, weight_hbm, target_hbm,
    both_ref, norm_ref, part0,
    mat, cost, lob, hib, cols, coef,
    base0, ai, ci, li, hi_i, lcb, sd, out, ri,
    sbuf, cbuf, rep, rbuf, sdo, idbuf, idin, hot, hot_t,
    rwt, den, memb, rows_new, res, resin, consin, gv, tab, tabs,
    lo_ref, hi_ref, iface, sub, live_ref, weight, target, bnd,
    in_sem, arg_sem, tab_sem, id_s, id_r, c_s, c_r, r_s, r_r, n_s, n_r, k_s, k_r,
):
    x, z, y, c = [lax.axis_index(a) for a in AXES]
    me = ((x * 4 + z) * 4 + y) * 2 + c
    k_me = x * 4 + z
    place = lax.rem(y - x - z + 8, 4)
    own = (c == 1) & (place < OWNERS)
    part = jnp.where(place < OWNERS, place, 0)

    def peer(dx, dz, dy, dc):
        t = (lax.rem(x + dx, 4), lax.rem(z + dz, 4), lax.rem(y + dy, 4), lax.rem(c + dc, 2))
        return t, ((t[0] * 4 + t[1]) * 4 + t[2]) * 2 + t[3]

    def wait(view, sem):
        pltpu.make_async_copy(view, view, sem).wait()

    small = [
        pltpu.make_async_copy(a, b, arg_sem.at[i])
        for i, (a, b) in enumerate(
            (
                (sub_hbm, sub),
                (live_hbm, live_ref),
                (iface_hbm, iface),
                (weight_hbm, weight),
                (lo_hbm, lo_ref),
                (hi_hbm, hi_ref),
                (target_hbm, target),
            )
        )
    ]

    def loads(j):
        s = pl.ds(j * CHUNK, CHUNK)
        return (
            pltpu.make_async_copy(inv_hbm.at[s], mat.at[s, pl.ds(0, K), :], in_sem.at[0, j]),
            pltpu.make_async_copy(cost_hbm.at[s], cost.at[s], in_sem.at[1, j]),
        )

    for copy in small[:3]:
        copy.start()
    for j in range(F // CHUNK):
        for copy in loads(j):
            copy.start()
    for copy in small[3:]:
        copy.start()
    barrier = pltpu.get_barrier_semaphore()
    for d in ALL:
        pl.semaphore_signal(barrier, inc=1, device_id=peer(*d)[0], device_id_type=MESH)

    for copy in small[:3]:
        copy.wait()
    live = live_ref[0]

    gv[...] = lax.broadcasted_iota(i32, (C, C), 0) + 1024
    for f in range(F):
        g = jnp.where(f < live, sub[f] // 32, 64 + f)
        gv[f : f + 1, :] = jnp.full((1, C), g, i32)
    grp = gv[...]
    grp_t = grp.T
    row = lax.broadcasted_iota(i32, (C, C), 0)
    lane = lax.broadcasted_iota(i32, (C, C), 1)
    same = grp == grp_t
    rank = jnp.sum(jnp.where(same & (row < lane), 1, 0), axis=0, keepdims=True)
    pos_row = grp_t[0:1] * 3 + rank
    here = jnp.broadcast_to(pos_row, (C, C)).T == lane
    slot_row = jnp.sum(jnp.where(here, row - F, 0), axis=0, keepdims=True) + F
    pos_row = jnp.minimum(pos_row, 47)
    tab[0:1, :] = slot_row
    tab[1:2, :] = pos_row
    to_smem = pltpu.make_async_copy(tab, tabs, tab_sem)
    to_smem.start()

    zero8 = jnp.zeros((F, 8, C), f32)
    for ref in (base0, ai, ci, li, hi_i, lcb, sd):
        ref[...] = zero8
    coef[...] = jnp.zeros((F, Q, 8, C), f32)
    out[F] = jnp.zeros((8, C), f32)
    def slot_at(n):
        return jnp.clip(tabs[0, n], 0, F)

    def to_owners(source, dest, first, s_sem, r_sem, self_copy):
        for dx, dz in PLANE:
            tx, tz = lax.rem(x + dx, 4), lax.rem(z + dz, 4)
            k = tx * 4 + tz
            for o in (2, 1, 0):
                ty = lax.rem(tx + tz + o, 4)
                copy = pltpu.make_async_remote_copy(
                    source(o, k),
                    dest.at[pl.ds(first + me * 6, 6), :],
                    s_sem,
                    r_sem,
                    device_id=(tx, tz, ty, 1),
                    device_id_type=MESH,
                )
                if (dx, dz) == (0, 0):
                    pl.when(jnp.logical_not((y == ty) & (c == 1)))(copy.start)
                else:
                    copy.start()

        @pl.when(own)
        def _():
            self_copy()

    def wait_48(view, sem):
        @pl.when(own)
        def _():
            wait(view.at[pl.ds(0, 47 * 6), :], sem)

        @pl.when(jnp.logical_not(own))
        def _():
            wait(view.at[pl.ds(0, 48 * 6), :], sem)

    lane16 = lax.broadcasted_iota(i32, (16, K), 1)
    row16 = lax.broadcasted_iota(i32, (16, K), 0)

    def picks(f):
        at = jnp.full((16, K), -1, i32)
        for q in range(Q):
            at = jnp.where(row16 == q, iface[q, f], at)
        pick = jnp.where(lane16 == at, 1.0, 0.0)
        return pick.astype(bf16), 1.0 - jnp.sum(pick, axis=0, keepdims=True)

    def prepare(f):
        part0[f] = mm(mat[f, 0:K, :], (-cost[f]).astype(bf16))
        for q in range(Q):
            base0[f, q : q + 1, :] = part0[f, pl.ds(iface[q, f], 1), :]

    def complete(f):
        pick, keep = picks(f)
        cols[f] = mm(mat[f, 0:K, :], pick, NT).astype(bf16)
        rows = mm(pick, mat[f, 0:K, :]).astype(bf16)
        cross = mm(rows, pick, NT)
        mat[f, K : K + 16, :] = rows * keep.astype(bf16)
        for q in range(Q):
            coef[f, q] = jnp.broadcast_to(cross[0:8, q : q + 1], (8, C))
        lob[f] = jnp.broadcast_to(lo_ref[pl.ds(f, 1), :], (C, K)).T
        hib[f] = jnp.broadcast_to(hi_ref[pl.ds(f, 1), :], (C, K)).T
        for q in range(Q):
            r = iface[q, f]
            ci[f, q : q + 1, :] = cost[f, pl.ds(r, 1), :]
            li[f, q : q + 1, :] = lob[f, pl.ds(r, 1), :]
            hi_i[f, q : q + 1, :] = hib[f, pl.ds(r, 1), :]

    def first(f):
        _, keep = picks(f)
        mat[f, 0:K, :] = mat[f, 0:K, :] * keep.astype(bf16)
        anchor = jnp.minimum(jnp.maximum(part0[f], lob[f]), hib[f])
        solve(f, (anchor - cost[f]).astype(bf16))

    def solve(f, base):
        both = mm(mat[f], base)
        part0[f] = both[0:K]
        base0[f] = both[K : K + 8]

    def chunk_loop(body, arrive=False):
        def step(j, carry):
            if arrive:
                for copy in loads(j):
                    copy.wait()
            for i in range(CHUNK):
                body(j * CHUNK + i)
            return carry

        lax.fori_loop(0, F // CHUNK, step, 0)

    chunk_loop(prepare, arrive=True)

    to_smem.wait()
    for n in range(48):
        s = slot_at(n)
        number = jnp.where(s < F, (sub[jnp.minimum(s, F - 1)] % 32).astype(f32), -1000.0)
        idbuf[2 * n : 2 * n + 1, :] = jnp.full((1, C), number, f32)
        idbuf[2 * n + 1 : 2 * n + 2, :] = jnp.full((1, C), number + 32.0, f32)
    pl.semaphore_wait(barrier, 127)

    def id_self():
        for i in range(6):
            idin[pl.ds(me * 6 + i, 1), :] = idbuf[pl.ds(k_me * 6 + i, 1), :]

    to_owners(lambda o, k: idbuf.at[pl.ds(k * 6, 6), :], idin, 0, id_s, id_r, id_self)
    for copy in small[3:]:
        copy.wait()

    def exchange(t):
        half_at = pl.multiple_of(lax.rem(t, 2) * 768, 768)
        for f in range(F):
            act = jnp.where(f < live, 1.0, 0.0)
            rhs = (ai[f] + PENALTY * (lcb[f] - sd[f])).astype(bf16).astype(f32)
            ri[f] = rhs
            boundary = base0[f]
            for q in range(Q):
                boundary = boundary + coef[f, q] * jnp.broadcast_to(rhs[q : q + 1, :], (8, C))
            out[f] = (boundary + sd[f]) * act
            bnd[f] = boundary
        for n in range(48):
            v = out[slot_at(n)]
            for o in range(OWNERS):
                sbuf[96 * o + 2 * n : 96 * o + 2 * n + 2, :] = v[2 * o : 2 * o + 2, :]

        def self_copy():
            for i in range(6):
                cbuf[pl.ds(half_at + me * 6 + i, 1), :] = sbuf[pl.ds(part * 96 + k_me * 6 + i, 1), :]

        to_owners(
            lambda o, k: sbuf.at[pl.ds(o * 96 + k * 6, 6), :], cbuf, half_at, c_s, c_r, self_copy
        )

        def primal_of(f):
            primal = part0[f] + mm(cols[f, :, 0:8], ri[f].astype(bf16))
            return jnp.minimum(jnp.maximum(primal, lob[f]), hib[f])

        @pl.when(t == 0)
        def _():
            chunk_loop(complete)

        @pl.when((t > 0) & (t < ITERS - 1))
        def _():
            def advance(f):
                solve(f, (primal_of(f) - cost[f]).astype(bf16))

            chunk_loop(advance)

        @pl.when(t == ITERS - 1)
        def _():
            def last(f):
                part0[f] = primal_of(f) * jnp.where(f < live, 1.0, 0.0)

            chunk_loop(last)

        @pl.when(own & (t == 0))
        def _():
            wait(idin.at[pl.ds(0, 127 * 6), :], id_r)
            lanes = lax.broadcasted_iota(i32, (768, 256), 1)
            want = jnp.where(lanes < 192, lax.rem(lanes, 64), -1).astype(f32)
            ids = idin[...]
            h = jnp.where(jnp.concatenate([ids, ids], axis=1) == want, 1.0, 0.0)
            hot[...] = h.astype(bf16)
            ht = h[:, 0:C].T[0:64, :]
            hot_t[...] = ht.astype(bf16)
            count = mm(ht.astype(bf16), jnp.ones((768, C), bf16))
            memb[...] = count
            for s in range(32):
                w = weight[s]
                for q in range(2):
                    r = s + 32 * q
                    rwt[r : r + 1, :] = w * target[2 * part + q, s : s + 1, :]
                    den[r : r + 1, :] = memb[r : r + 1, :] + w
            sdo[...] = jnp.zeros((768, C), f32)
            rows_new[...] = jnp.zeros((64, C), f32)
            res[...] = jnp.zeros((1, C), f32)

        for f in range(F):
            ai[f] = jnp.minimum(jnp.maximum(bnd[f], li[f]), hi_i[f]) - ci[f]

        @pl.when(own)
        def _():
            wait(cbuf.at[pl.ds(half_at, 127 * 6), :], c_r)
            arrived = cbuf.at[pl.ds(half_at, 768), :]
            sums = None
            for a in parts(arrived[...]):
                term = mm(hot_t[...], a)
                sums = term if sums is None else sums + term
            new = (sums + rwt[...]) / den[...]
            diff = new - rows_new[...]
            rows_new[...] = new
            triple = jnp.concatenate([*parts(new), jnp.zeros((64, C), bf16)], axis=0)
            back = mm(hot[...], triple)
            rep[...] = back
            for d in ALL:
                to, number = peer(*d)
                pltpu.make_async_remote_copy(
                    rep.at[pl.ds(number * 6, 6), :],
                    rbuf.at[pl.ds(part * 96 + k_me * 6, 6), :],
                    r_s,
                    r_r,
                    device_id=to,
                    device_id_type=MESH,
                ).start()
            for i in range(6):
                rbuf[pl.ds(part * 96 + k_me * 6 + i, 1), :] = rep[pl.ds(me * 6 + i, 1), :]
            next_sd = arrived[...] - rep[...]
            miss = next_sd - sdo[...]
            sdo[...] = next_sd
            primal_sum = jnp.sum(miss * miss, axis=0, keepdims=True)
            dual_sum = jnp.sum(memb[...] * (diff * diff), axis=0, keepdims=True)
            lane1 = lax.broadcasted_iota(i32, (1, C), 1)
            for at, value in ((t, primal_sum), (t + 64, dual_sum)):
                value = jnp.broadcast_to(jnp.sum(value, axis=1, keepdims=True), (1, C))
                res[...] = jnp.where(lane1 == at, value, res[...])

            @pl.when(t == ITERS - 1)
            def _():
                for dx, dz, dy, dc in ALL:
                    to, number = peer(dx, dz, dy, dc)
                    if (dx, dz) == (0, 0):
                        pltpu.make_async_remote_copy(
                            rows_new, consin.at[part], k_s, k_r, device_id=to, device_id_type=MESH
                        ).start()
                    pltpu.make_async_remote_copy(
                        res, resin.at[pl.ds(part * 16 + k_me, 1), :], n_s, n_r, device_id=to, device_id_type=MESH
                    ).start()
                resin[pl.ds(part * 16 + k_me, 1), :] = res[...]
                consin[part] = rows_new[...]

            wait(rep.at[pl.ds(0, 127 * 6), :], r_s)

        @pl.when(t == 0)
        def _():
            chunk_loop(first)

        wait_48(rbuf, r_r)

        for f in range(F):
            at = 2 * jnp.clip(tabs[1, f], 0, 47)
            for o in range(OWNERS):
                for q in range(2):
                    r = 2 * o + q
                    lcb[f, r : r + 1, :] = rbuf[pl.ds(96 * o + at + q, 1), :]
        for f in range(F):
            act = jnp.where(f < live, 1.0, 0.0)
            sd[f] = out[f] - lcb[f] * act

        wait_48(sbuf, c_s)
        return 0

    lax.fori_loop(0, ITERS, lambda t, carry: exchange(t), 0)

    for q in range(Q):
        both_ref[q] = PENALTY * sd[:, q, :]

    @pl.when(own)
    def _():
        wait(consin.at[pl.ds(0, 2)], k_r)
        wait(resin.at[pl.ds(0, 47), :], n_r)

    @pl.when(jnp.logical_not(own))
    def _():
        wait(consin, k_r)
        wait(resin, n_r)

    for o in range(OWNERS):
        for q in range(2):
            both_ref[Q + 2 * o + q] = consin[o, 32 * q : 32 * q + 32, :]
    root = jnp.sqrt(jnp.sum(resin[...], axis=0, keepdims=True))
    norm_ref[0:1, :] = root[:, 0:ITERS]
    norm_ref[1:2, :] = PENALTY * root[:, 64 : 64 + ITERS]

    @pl.when(own)
    def _():
        wait(cbuf.at[pl.ds(0, 7 * 64), :], k_s)
        wait(cbuf.at[pl.ds(0, 127), :], n_s)

    wait_48(idin, id_s)


def shards(inverse, cost, lower, upper, iface, sub, live, weight, target):
    operands = (inverse, cost, lower, upper, iface.T, sub, live, weight, target.transpose(1, 0, 2))
    vmem = functools.partial(pltpu.VMEM, dtype=f32)
    anyspace = pl.BlockSpec(memory_space=pl.ANY)
    on_vmem = pl.BlockSpec(memory_space=pltpu.VMEM)
    dma = pltpu.SemaphoreType.DMA
    shapes = ((2 * Q, F, C), (2, ITERS), (F, K, C))
    both, norms, setpoints = pl.pallas_call(
        kernel,
        out_shape=tuple(vmem(shape) for shape in shapes),
        in_specs=[anyspace] * 9,
        out_specs=(on_vmem,) * 3,
        scratch_shapes=[
            pltpu.VMEM((F, K + 16, K), bf16),
            vmem((F, K, C)),
            vmem((F, K, C)),
            vmem((F, K, C)),
            pltpu.VMEM((F, K, 16), bf16),
            vmem((F, Q, 8, C)),
            vmem((F, 8, C)),
            vmem((F, 8, C)),
            vmem((F, 8, C)),
            vmem((F, 8, C)),
            vmem((F, 8, C)),
            vmem((F, 8, C)),
            vmem((F, 8, C)),
            vmem((F + 1, 8, C)),
            vmem((F, 8, C)),
            vmem((OWNERS * 96, C)),
            vmem((2 * 768, C)),
            vmem((768, C)),
            vmem((OWNERS * 96, C)),
            vmem((768, C)),
            vmem((96, C)),
            vmem((768, C)),
            pltpu.VMEM((768, 256), bf16),
            pltpu.VMEM((64, 768), bf16),
            vmem((64, C)),
            vmem((64, C)),
            vmem((64, C)),
            vmem((64, C)),
            vmem((1, C)),
            vmem((48, C)),
            vmem((OWNERS, 64, C)),
            pltpu.VMEM((C, C), i32),
            pltpu.VMEM((2, C), i32),
            pltpu.SMEM((2, C), i32),
            vmem((F, K)),
            vmem((F, K)),
            pltpu.SMEM((Q, F), i32),
            pltpu.SMEM((F,), i32),
            pltpu.SMEM((1,), i32),
            pltpu.SMEM((32,), f32),
            vmem((Q, 32, C)),
            vmem((F, 8, C)),
            dma((2, F // CHUNK)),
            dma((7,)),
            dma,
            dma,
            dma,
            dma,
            dma,
            dma,
            dma,
            dma,
            dma,
            dma,
            dma,
        ],
        compiler_params=pltpu.CompilerParams(
            collective_id=0, has_side_effects=True, vmem_limit_bytes=58 * 2**20
        ),
    )(*operands)
    duals, consensus = both[:Q], both[Q:]
    return duals.transpose(1, 0, 2), consensus.transpose(1, 0, 2), norms.T, setpoints


def solution(mesh):
    torus = Mesh(mesh.devices.reshape(4, 4, 4, 2), AXES)
    placed = (
        P(AXES, None, None),
        P(AXES, None, None),
        P(AXES, None),
        P(AXES, None),
        P(AXES, None),
        P(AXES),
        P(AXES),
        P(SUB),
        P(SUB, None, None),
    )
    return jax.shard_map(
        shards,
        mesh=torus,
        in_specs=placed,
        out_specs=(P(AXES, None, None), P(SUB, None, None), P(), P(AXES, None, None)),
        check_vma=False,
    )
```

```python
import functools

import jax
import jax.numpy as jnp
from jax import lax
from jax.experimental import pallas as pl
from jax.experimental.pallas import tpu as pltpu
from jax.sharding import Mesh
from jax.sharding import PartitionSpec as P


ITERS = 5
PENALTY = 2.0
AXES = ("sub_0", "sub_1", "fdr_0", "fdr_1")
SUB = ("sub_0", "sub_1")
F, K, C, Q = 32, 256, 128, 6
OWNERS = 3
CHUNK = 8
MESH = pl.DeviceIdType.MESH
NT = (((1,), (1,)), ((), ()))
f32, bf16, i32 = jnp.float32, jnp.bfloat16, jnp.int32


def ring(d):
    return min(d, 4 - d)


PLANE = sorted(
    ((dx, dz) for dx in range(4) for dz in range(4)),
    key=lambda t: -(ring(t[0]) + ring(t[1])),
)
ALL = sorted(
    (
        (dx, dz, dy, dc)
        for dx in range(4)
        for dz in range(4)
        for dy in range(4)
        for dc in range(2)
    ),
    key=lambda t: -(ring(t[0]) + ring(t[1]) + ring(t[2])),
)[:-2] + [(0, 0, 0, 1)]


def parts(v):
    hi = v.astype(bf16)
    rest = v - hi.astype(f32)
    mid = rest.astype(bf16)
    low = (rest - mid.astype(f32)).astype(bf16)
    return hi, mid, low


def mm(a, b, dims=(((1,), (0,)), ((), ()))):
    return lax.dot_general(a, b, dims, preferred_element_type=f32)


def kernel(
    inv_hbm, cost_hbm, lo_hbm, hi_hbm, iface_hbm, sub_hbm, live_hbm, weight_hbm, target_hbm,
    both_ref, norm_ref, part0,
    mat, cost, lob, hib, cols, coef,
    base0, ai, ci, li, hi_i, lcb, sd, out, ri,
    sbuf, cbuf, rep, rbuf, sdo, idbuf, idin, hot, hot_t,
    rwt, den, memb, rows_new, res, resin, consin, gv, tab, tabs,
    lo_ref, hi_ref, iface, sub, live_ref, weight, target, bnd,
    in_sem, arg_sem, tab_sem, id_s, id_r, c_s, c_r, r_s, r_r, n_s, n_r, k_s, k_r,
):
    x, z, y, c = [lax.axis_index(a) for a in AXES]
    me = ((x * 4 + z) * 4 + y) * 2 + c
    k_me = x * 4 + z
    place = lax.rem(y - x - z + 8, 4)
    own = (c == 1) & (place < OWNERS)
    part = jnp.where(place < OWNERS, place, 0)

    def peer(dx, dz, dy, dc):
        t = (lax.rem(x + dx, 4), lax.rem(z + dz, 4), lax.rem(y + dy, 4), lax.rem(c + dc, 2))
        return t, ((t[0] * 4 + t[1]) * 4 + t[2]) * 2 + t[3]

    def wait(view, sem):
        pltpu.make_async_copy(view, view, sem).wait()

    small = [
        pltpu.make_async_copy(a, b, arg_sem.at[i])
        for i, (a, b) in enumerate(
            (
                (sub_hbm, sub),
                (live_hbm, live_ref),
                (iface_hbm, iface),
                (weight_hbm, weight),
                (lo_hbm, lo_ref),
                (hi_hbm, hi_ref),
                (target_hbm, target),
            )
        )
    ]

    def loads(j):
        s = pl.ds(j * CHUNK, CHUNK)
        return (
            pltpu.make_async_copy(inv_hbm.at[s], mat.at[s, pl.ds(0, K), :], in_sem.at[0, j]),
            pltpu.make_async_copy(cost_hbm.at[s], cost.at[s], in_sem.at[1, j]),
        )

    for copy in small[:3]:
        copy.start()
    for j in range(F // CHUNK):
        for copy in loads(j):
            copy.start()
    for copy in small[3:]:
        copy.start()
    barrier = pltpu.get_barrier_semaphore()
    for d in ALL:
        pl.semaphore_signal(barrier, inc=1, device_id=peer(*d)[0], device_id_type=MESH)

    for copy in small[:3]:
        copy.wait()
    live = live_ref[0]

    gv[...] = lax.broadcasted_iota(i32, (C, C), 0) + 1024
    for f in range(F):
        g = jnp.where(f < live, sub[f] // 32, 64 + f)
        gv[f : f + 1, :] = jnp.full((1, C), g, i32)
    grp = gv[...]
    grp_t = grp.T
    row = lax.broadcasted_iota(i32, (C, C), 0)
    lane = lax.broadcasted_iota(i32, (C, C), 1)
    same = grp == grp_t
    rank = jnp.sum(jnp.where(same & (row < lane), 1, 0), axis=0, keepdims=True)
    pos_row = grp_t[0:1] * 3 + rank
    here = jnp.broadcast_to(pos_row, (C, C)).T == lane
    slot_row = jnp.sum(jnp.where(here, row - F, 0), axis=0, keepdims=True) + F
    pos_row = jnp.minimum(pos_row, 47)
    tab[0:1, :] = slot_row
    tab[1:2, :] = pos_row
    to_smem = pltpu.make_async_copy(tab, tabs, tab_sem)
    to_smem.start()

    zero8 = jnp.zeros((F, 8, C), f32)
    for ref in (base0, ai, ci, li, hi_i, lcb, sd):
        ref[...] = zero8
    coef[...] = jnp.zeros((F, Q, 8, C), f32)
    out[F] = jnp.zeros((8, C), f32)
    def slot_at(n):
        return jnp.clip(tabs[0, n], 0, F)

    def to_owners(source, dest, first, s_sem, r_sem, self_copy):
        for dx, dz in PLANE:
            tx, tz = lax.rem(x + dx, 4), lax.rem(z + dz, 4)
            k = tx * 4 + tz
            for o in (2, 1, 0):
                ty = lax.rem(tx + tz + o, 4)
                copy = pltpu.make_async_remote_copy(
                    source(o, k),
                    dest.at[pl.ds(first + me * 6, 6), :],
                    s_sem,
                    r_sem,
                    device_id=(tx, tz, ty, 1),
                    device_id_type=MESH,
                )
                if (dx, dz) == (0, 0):
                    pl.when(jnp.logical_not((y == ty) & (c == 1)))(copy.start)
                else:
                    copy.start()

        @pl.when(own)
        def _():
            self_copy()

    def wait_48(view, sem):
        @pl.when(own)
        def _():
            wait(view.at[pl.ds(0, 47 * 6), :], sem)

        @pl.when(jnp.logical_not(own))
        def _():
            wait(view.at[pl.ds(0, 48 * 6), :], sem)

    lane16 = lax.broadcasted_iota(i32, (16, K), 1)
    row16 = lax.broadcasted_iota(i32, (16, K), 0)

    def picks(f):
        at = jnp.full((16, K), -1, i32)
        for q in range(Q):
            at = jnp.where(row16 == q, iface[q, f], at)
        pick = jnp.where(lane16 == at, 1.0, 0.0)
        return pick.astype(bf16), 1.0 - jnp.sum(pick, axis=0, keepdims=True)

    def prepare(f):
        part0[f] = mm(mat[f, 0:K, :], (-cost[f]).astype(bf16))
        for q in range(Q):
            base0[f, q : q + 1, :] = part0[f, pl.ds(iface[q, f], 1), :]

    def complete(f):
        pick, keep = picks(f)
        cols[f] = mm(mat[f, 0:K, :], pick, NT).astype(bf16)
        rows = mm(pick, mat[f, 0:K, :]).astype(bf16)
        cross = mm(rows, pick, NT)
        mat[f, K : K + 16, :] = rows * keep.astype(bf16)
        for q in range(Q):
            coef[f, q] = jnp.broadcast_to(cross[0:8, q : q + 1], (8, C))
        lob[f] = jnp.broadcast_to(lo_ref[pl.ds(f, 1), :], (C, K)).T
        hib[f] = jnp.broadcast_to(hi_ref[pl.ds(f, 1), :], (C, K)).T
        for q in range(Q):
            r = iface[q, f]
            ci[f, q : q + 1, :] = cost[f, pl.ds(r, 1), :]
            li[f, q : q + 1, :] = lob[f, pl.ds(r, 1), :]
            hi_i[f, q : q + 1, :] = hib[f, pl.ds(r, 1), :]

    def first(f):
        _, keep = picks(f)
        mat[f, 0:K, :] = mat[f, 0:K, :] * keep.astype(bf16)
        anchor = jnp.minimum(jnp.maximum(part0[f], lob[f]), hib[f])
        solve(f, (anchor - cost[f]).astype(bf16))

    def solve(f, base):
        both = mm(mat[f], base)
        part0[f] = both[0:K]
        base0[f] = both[K : K + 8]

    def chunk_loop(body, arrive=False):
        def step(j, carry):
            if arrive:
                for copy in loads(j):
                    copy.wait()
            for i in range(CHUNK):
                body(j * CHUNK + i)
            return carry

        lax.fori_loop(0, F // CHUNK, step, 0)

    chunk_loop(prepare, arrive=True)

    to_smem.wait()
    for n in range(48):
        s = slot_at(n)
        number = jnp.where(s < F, (sub[jnp.minimum(s, F - 1)] % 32).astype(f32), -1000.0)
        idbuf[2 * n : 2 * n + 1, :] = jnp.full((1, C), number, f32)
        idbuf[2 * n + 1 : 2 * n + 2, :] = jnp.full((1, C), number + 32.0, f32)
    pl.semaphore_wait(barrier, 127)

    def id_self():
        for i in range(6):
            idin[pl.ds(me * 6 + i, 1), :] = idbuf[pl.ds(k_me * 6 + i, 1), :]

    to_owners(lambda o, k: idbuf.at[pl.ds(k * 6, 6), :], idin, 0, id_s, id_r, id_self)
    for copy in small[3:]:
        copy.wait()

    def exchange(t):
        half_at = pl.multiple_of(lax.rem(t, 2) * 768, 768)
        for f in range(F):
            act = jnp.where(f < live, 1.0, 0.0)
            rhs = (ai[f] + PENALTY * (lcb[f] - sd[f])).astype(bf16).astype(f32)
            ri[f] = rhs
            boundary = base0[f]
            for q in range(Q):
                boundary = boundary + coef[f, q] * jnp.broadcast_to(rhs[q : q + 1, :], (8, C))
            out[f] = (boundary + sd[f]) * act
            bnd[f] = boundary
        for n in range(48):
            v = out[slot_at(n)]
            for o in range(OWNERS):
                sbuf[96 * o + 2 * n : 96 * o + 2 * n + 2, :] = v[2 * o : 2 * o + 2, :]

        def self_copy():
            for i in range(6):
                cbuf[pl.ds(half_at + me * 6 + i, 1), :] = sbuf[pl.ds(part * 96 + k_me * 6 + i, 1), :]

        to_owners(
            lambda o, k: sbuf.at[pl.ds(o * 96 + k * 6, 6), :], cbuf, half_at, c_s, c_r, self_copy
        )

        def primal_of(f):
            primal = part0[f] + mm(cols[f, :, 0:8], ri[f].astype(bf16))
            return jnp.minimum(jnp.maximum(primal, lob[f]), hib[f])

        @pl.when(t == 0)
        def _():
            chunk_loop(complete)

        @pl.when((t > 0) & (t < ITERS - 1))
        def _():
            def advance(f):
                solve(f, (primal_of(f) - cost[f]).astype(bf16))

            chunk_loop(advance)

        @pl.when(t == ITERS - 1)
        def _():
            def last(f):
                part0[f] = primal_of(f) * jnp.where(f < live, 1.0, 0.0)

            chunk_loop(last)

        @pl.when(own & (t == 0))
        def _():
            wait(idin.at[pl.ds(0, 127 * 6), :], id_r)
            lanes = lax.broadcasted_iota(i32, (768, 256), 1)
            want = jnp.where(lanes < 192, lax.rem(lanes, 64), -1).astype(f32)
            ids = idin[...]
            h = jnp.where(jnp.concatenate([ids, ids], axis=1) == want, 1.0, 0.0)
            hot[...] = h.astype(bf16)
            ht = h[:, 0:C].T[0:64, :]
            hot_t[...] = ht.astype(bf16)
            count = mm(ht.astype(bf16), jnp.ones((768, C), bf16))
            memb[...] = count
            for s in range(32):
                w = weight[s]
                for q in range(2):
                    r = s + 32 * q
                    rwt[r : r + 1, :] = w * target[2 * part + q, s : s + 1, :]
                    den[r : r + 1, :] = memb[r : r + 1, :] + w
            sdo[...] = jnp.zeros((768, C), f32)
            rows_new[...] = jnp.zeros((64, C), f32)
            res[...] = jnp.zeros((1, C), f32)

        for f in range(F):
            ai[f] = jnp.minimum(jnp.maximum(bnd[f], li[f]), hi_i[f]) - ci[f]

        @pl.when(own)
        def _():
            wait(cbuf.at[pl.ds(half_at, 127 * 6), :], c_r)
            arrived = cbuf.at[pl.ds(half_at, 768), :]
            sums = None
            for a in parts(arrived[...]):
                term = mm(hot_t[...], a)
                sums = term if sums is None else sums + term
            new = (sums + rwt[...]) / den[...]
            diff = new - rows_new[...]
            rows_new[...] = new
            triple = jnp.concatenate([*parts(new), jnp.zeros((64, C), bf16)], axis=0)
            back = mm(hot[...], triple)
            rep[...] = back
            for d in ALL:
                to, number = peer(*d)
                pltpu.make_async_remote_copy(
                    rep.at[pl.ds(number * 6, 6), :],
                    rbuf.at[pl.ds(part * 96 + k_me * 6, 6), :],
                    r_s,
                    r_r,
                    device_id=to,
                    device_id_type=MESH,
                ).start()
            for i in range(6):
                rbuf[pl.ds(part * 96 + k_me * 6 + i, 1), :] = rep[pl.ds(me * 6 + i, 1), :]

            @pl.when(t == ITERS - 1)
            def _():
                for d in ALL:
                    if d[:2] == (0, 0):
                        pltpu.make_async_remote_copy(
                            rows_new,
                            consin.at[part],
                            k_s,
                            k_r,
                            device_id=peer(*d)[0],
                            device_id_type=MESH,
                        ).start()

            next_sd = arrived[...] - rep[...]
            miss = next_sd - sdo[...]
            sdo[...] = next_sd
            primal_sum = jnp.sum(miss * miss, axis=0, keepdims=True)
            dual_sum = jnp.sum(memb[...] * (diff * diff), axis=0, keepdims=True)
            lane1 = lax.broadcasted_iota(i32, (1, C), 1)
            for at, value in ((t, primal_sum), (t + 64, dual_sum)):
                value = jnp.broadcast_to(jnp.sum(value, axis=1, keepdims=True), (1, C))
                res[...] = jnp.where(lane1 == at, value, res[...])

            @pl.when(t == ITERS - 1)
            def _():
                for dx, dz, dy, dc in ALL:
                    to, number = peer(dx, dz, dy, dc)
                    pltpu.make_async_remote_copy(
                        res, resin.at[pl.ds(part * 16 + k_me, 1), :], n_s, n_r, device_id=to, device_id_type=MESH
                    ).start()
                resin[pl.ds(part * 16 + k_me, 1), :] = res[...]
                consin[part] = rows_new[...]

            wait(rep.at[pl.ds(0, 127 * 6), :], r_s)

        @pl.when(t == 0)
        def _():
            chunk_loop(first)

        wait_48(rbuf, r_r)

        for f in range(F):
            at = 2 * jnp.clip(tabs[1, f], 0, 47)
            for o in range(OWNERS):
                for q in range(2):
                    r = 2 * o + q
                    lcb[f, r : r + 1, :] = rbuf[pl.ds(96 * o + at + q, 1), :]
        for f in range(F):
            act = jnp.where(f < live, 1.0, 0.0)
            sd[f] = out[f] - lcb[f] * act

        wait_48(sbuf, c_s)
        return 0

    lax.fori_loop(0, ITERS, lambda t, carry: exchange(t), 0)

    for q in range(Q):
        both_ref[q] = PENALTY * sd[:, q, :]

    @pl.when(own)
    def _():
        wait(consin.at[pl.ds(0, 2)], k_r)
        wait(resin.at[pl.ds(0, 47), :], n_r)

    @pl.when(jnp.logical_not(own))
    def _():
        wait(consin, k_r)
        wait(resin, n_r)

    for o in range(OWNERS):
        for q in range(2):
            both_ref[Q + 2 * o + q] = consin[o, 32 * q : 32 * q + 32, :]
    root = jnp.sqrt(jnp.sum(resin[...], axis=0, keepdims=True))
    norm_ref[0:1, :] = root[:, 0:ITERS]
    norm_ref[1:2, :] = PENALTY * root[:, 64 : 64 + ITERS]

    @pl.when(own)
    def _():
        wait(cbuf.at[pl.ds(0, 7 * 64), :], k_s)
        wait(cbuf.at[pl.ds(0, 127), :], n_s)

    wait_48(idin, id_s)


def shards(inverse, cost, lower, upper, iface, sub, live, weight, target):
    operands = (inverse, cost, lower, upper, iface.T, sub, live, weight, target.transpose(1, 0, 2))
    vmem = functools.partial(pltpu.VMEM, dtype=f32)
    anyspace = pl.BlockSpec(memory_space=pl.ANY)
    on_vmem = pl.BlockSpec(memory_space=pltpu.VMEM)
    dma = pltpu.SemaphoreType.DMA
    shapes = ((2 * Q, F, C), (2, ITERS), (F, K, C))
    both, norms, setpoints = pl.pallas_call(
        kernel,
        out_shape=tuple(vmem(shape) for shape in shapes),
        in_specs=[anyspace] * 9,
        out_specs=(on_vmem,) * 3,
        scratch_shapes=[
            pltpu.VMEM((F, K + 16, K), bf16),
            vmem((F, K, C)),
            vmem((F, K, C)),
            vmem((F, K, C)),
            pltpu.VMEM((F, K, 16), bf16),
            vmem((F, Q, 8, C)),
            vmem((F, 8, C)),
            vmem((F, 8, C)),
            vmem((F, 8, C)),
            vmem((F, 8, C)),
            vmem((F, 8, C)),
            vmem((F, 8, C)),
            vmem((F, 8, C)),
            vmem((F + 1, 8, C)),
            vmem((F, 8, C)),
            vmem((OWNERS * 96, C)),
            vmem((2 * 768, C)),
            vmem((768, C)),
            vmem((OWNERS * 96, C)),
            vmem((768, C)),
            vmem((96, C)),
            vmem((768, C)),
            pltpu.VMEM((768, 256), bf16),
            pltpu.VMEM((64, 768), bf16),
            vmem((64, C)),
            vmem((64, C)),
            vmem((64, C)),
            vmem((64, C)),
            vmem((1, C)),
            vmem((48, C)),
            vmem((OWNERS, 64, C)),
            pltpu.VMEM((C, C), i32),
            pltpu.VMEM((2, C), i32),
            pltpu.SMEM((2, C), i32),
            vmem((F, K)),
            vmem((F, K)),
            pltpu.SMEM((Q, F), i32),
            pltpu.SMEM((F,), i32),
            pltpu.SMEM((1,), i32),
            pltpu.SMEM((32,), f32),
            vmem((Q, 32, C)),
            vmem((F, 8, C)),
            dma((2, F // CHUNK)),
            dma((7,)),
            dma,
            dma,
            dma,
            dma,
            dma,
            dma,
            dma,
            dma,
            dma,
            dma,
            dma,
        ],
        compiler_params=pltpu.CompilerParams(
            collective_id=0, has_side_effects=True, vmem_limit_bytes=58 * 2**20
        ),
    )(*operands)
    duals, consensus = both[:Q], both[Q:]
    return duals.transpose(1, 0, 2), consensus.transpose(1, 0, 2), norms.T, setpoints


def solution(mesh):
    torus = Mesh(mesh.devices.reshape(4, 4, 4, 2), AXES)
    placed = (
        P(AXES, None, None),
        P(AXES, None, None),
        P(AXES, None),
        P(AXES, None),
        P(AXES, None),
        P(AXES),
        P(AXES),
        P(SUB),
        P(SUB, None, None),
    )
    return jax.shard_map(
        shards,
        mesh=torus,
        in_specs=placed,
        out_specs=(P(AXES, None, None), P(SUB, None, None), P(), P(AXES, None, None)),
        check_vma=False,
    )
```
